32 devices in a mesh: rep: 1 (over z), tp: 4 (over y), sp: 8 (over x, core).
Axes of the slice: x: 4, y: 4, z: 1, core: 2. Of those that a mesh axis runs over, the one named last changes fastest.
The devices are a block of a 4x4x8 slice.
Arguments:
- x_in: bfloat16 [8192, 4096], P(('rep', 'sp'))
- positions: int32 [8192], P(('rep', 'sp'))
- norm_gain: float32 [4096], replicated
- w_q: bfloat16 [4096, 4096], P(None, 'tp')
- w_k: bfloat16 [4096, 1024], P(None, 'tp')
- w_v: bfloat16 [4096, 1024], P(None, 'tp')
- w_o: bfloat16 [4096, 4096], P('tp')
- w_gate: bfloat16 [4096, 14336], P(None, 'tp')
- w_up: bfloat16 [4096, 14336], P(None, 'tp')
- w_down: bfloat16 [14336, 4096], P('tp')
Outputs:
- output 1: bfloat16 [8192, 4096], P(('rep', 'sp'))
- output 2: bfloat16 [8192, 32, 128], P('rep', ('tp', 'sp'))
- output 3: bfloat16 [8192, 32, 128], P('rep', ('tp', 'sp'))
All inputs are finite; a program needn't handle non-finite values.
Results may differ from the reference program's by a relative error of at most 0.00226143.
Values are sent between devices in bfloat16 or wider.
A program may use at most 768 MiB of HBM per device.

```python
import math
import jax
import jax.numpy as jnp
from jax import lax

MODEL_DIM = 4096
NUM_HEADS = 32
KV_HEADS = 8
HEAD_DIM = 128
FF_DIM = 14336
TOKENS = 8192
GROUP_DEVS = 32
DOC_COUNT = 8

KV_REPEAT = max(GROUP_DEVS // KV_HEADS, 1)
GROUP_SIZE = NUM_HEADS // KV_HEADS
ROW_BLOCK = min(TOKENS, 64)
NUM_BLOCKS = TOKENS // ROW_BLOCK
EPS = 1e-6
ROPE_BASE = 500000.0
SCORE_SCALE = 1.0 / math.sqrt(HEAD_DIM)


def setup_inputs(seed: int = 0, part: int = 0) -> dict:
    part_keys = jax.random.split(jax.random.fold_in(jax.random.key(seed), part), 3)
    shared_keys = jax.random.split(jax.random.key(seed + 1), 8)

    def weight(key_w, fan_in, fan_out):
        return (jax.random.normal(key_w, (fan_in, fan_out), jnp.float32) * fan_in ** -0.5).astype(jnp.bfloat16)

    noise_part = jax.random.normal(part_keys[0], (DOC_COUNT, TOKENS // DOC_COUNT, MODEL_DIM), jnp.float32)
    doc_means = jax.random.normal(part_keys[1], (DOC_COUNT, 1, MODEL_DIM), jnp.float32)
    x_in = (noise_part + doc_means).reshape(TOKENS, MODEL_DIM).astype(jnp.bfloat16)
    start_pos = jax.random.randint(part_keys[2], (), 0, TOKENS)
    positions = (start_pos + jnp.arange(TOKENS)).astype(jnp.int32)
    norm_gain = 1.0 + 0.3 * jax.random.normal(shared_keys[0], (MODEL_DIM,), jnp.float32)
    return {
        "x_in": x_in,
        "positions": positions,
        "norm_gain": norm_gain,
        "w_q": weight(shared_keys[1], MODEL_DIM, NUM_HEADS * HEAD_DIM),
        "w_k": weight(shared_keys[2], MODEL_DIM, KV_HEADS * HEAD_DIM),
        "w_v": weight(shared_keys[3], MODEL_DIM, KV_HEADS * HEAD_DIM),
        "w_o": weight(shared_keys[4], NUM_HEADS * HEAD_DIM, MODEL_DIM),
        "w_gate": weight(shared_keys[5], MODEL_DIM, FF_DIM),
        "w_up": weight(shared_keys[6], MODEL_DIM, FF_DIM),
        "w_down": weight(shared_keys[7], FF_DIM, MODEL_DIM),
    }


def rotate(vectors, cos_tab, sin_tab):
    half_dim = HEAD_DIM // 2
    lower_part = vectors[..., :half_dim]
    upper_part = vectors[..., half_dim:]
    return jnp.concatenate([lower_part * cos_tab - upper_part * sin_tab, upper_part * cos_tab + lower_part * sin_tab], axis=-1).astype(jnp.bfloat16)


def reference(x_in, positions, norm_gain, w_q, w_k, w_v, w_o, w_gate, w_up, w_down):
    x_f32 = x_in.astype(jnp.float32)
    inv_rms = lax.rsqrt(jnp.mean(x_f32 * x_f32, axis=-1, keepdims=True) + EPS)
    normed = (x_f32 * inv_rms * norm_gain).astype(jnp.bfloat16)
    inv_freq = ROPE_BASE ** (-(jnp.arange(HEAD_DIM // 2, dtype=jnp.float32) * (2.0 / HEAD_DIM)))
    angles = positions.astype(jnp.float32)[:, None] * inv_freq[None, :]
    cos_tab = jnp.cos(angles)[:, None, :]
    sin_tab = jnp.sin(angles)[:, None, :]
    q_rot = rotate(jnp.dot(normed, w_q, preferred_element_type=jnp.float32).reshape(TOKENS, NUM_HEADS, HEAD_DIM), cos_tab, sin_tab)
    k_rot = rotate(jnp.dot(normed, w_k, preferred_element_type=jnp.float32).reshape(TOKENS, KV_HEADS, HEAD_DIM), cos_tab, sin_tab)
    v_val = jnp.dot(normed, w_v, preferred_element_type=jnp.float32).astype(jnp.bfloat16).reshape(TOKENS, KV_HEADS, HEAD_DIM)
    q_grouped = q_rot.reshape(TOKENS, KV_HEADS, GROUP_SIZE, HEAD_DIM).astype(jnp.float32)
    k_f32 = k_rot.astype(jnp.float32)
    v_f32 = v_val.astype(jnp.float32)
    key_idx = jnp.arange(TOKENS)

    def attend_block(block_id):
        q_tile = lax.dynamic_slice_in_dim(q_grouped, block_id * ROW_BLOCK, ROW_BLOCK, axis=0)
        scores = jnp.einsum("qcgd,kcd->cgqk", q_tile, k_f32) * SCORE_SCALE
        query_idx = block_id * ROW_BLOCK + jnp.arange(ROW_BLOCK)
        scores = jnp.where(key_idx[None, :] <= query_idx[:, None], scores, -jnp.inf)
        weights = jnp.exp(scores - jnp.max(scores, axis=-1, keepdims=True))
        weight_total = jnp.sum(weights, axis=-1)
        weighted_sum = jnp.einsum("cgqk,kcd->qcgd", weights.astype(jnp.bfloat16).astype(jnp.float32), v_f32)
        return (weighted_sum / jnp.transpose(weight_total, (2, 0, 1))[..., None]).astype(jnp.bfloat16)

    attn_out = lax.map(attend_block, jnp.arange(NUM_BLOCKS)).reshape(TOKENS, NUM_HEADS * HEAD_DIM)
    attn_proj = jnp.dot(attn_out, w_o, preferred_element_type=jnp.float32)
    gate_acc = jnp.dot(normed, w_gate, preferred_element_type=jnp.float32)
    up_acc = jnp.dot(normed, w_up, preferred_element_type=jnp.float32)
    hidden = (jax.nn.silu(gate_acc) * up_acc).astype(jnp.bfloat16)
    mlp_out = jnp.dot(hidden, w_down, preferred_element_type=jnp.float32)
    y_out = (x_f32 + attn_proj + mlp_out).astype(jnp.bfloat16)
    k_cache = jnp.repeat(k_rot, KV_REPEAT, axis=1)
    v_cache = jnp.repeat(v_val, KV_REPEAT, axis=1)
    return y_out, k_cache, v_cache
```

```python
import functools
import math

import jax
import jax.numpy as jnp
from jax import lax
from jax.experimental import pallas as pl
from jax.experimental.pallas import tpu as pltpu
from jax.sharding import PartitionSpec as P

HEAD_DIM = 128
EPS = 1e-6
ROPE_BASE = 500000.0
SCORE_SCALE = HEAD_DIM ** -0.5
EXP2_SCALE = SCORE_SCALE * math.log2(math.e)
VMEM_LIMIT = 60 * 1024 * 1024
CHUNKS = 4
ROW_GROUP = 32


def rope_tables(positions):
    inv_freq = ROPE_BASE ** (-(jnp.arange(HEAD_DIM // 2, dtype=jnp.float32) * (2.0 / HEAD_DIM)))
    angles = positions.astype(jnp.float32)[:, None] * inv_freq[None, :]
    cos_tab, sin_tab = jnp.cos(angles), jnp.sin(angles)
    return jnp.concatenate([cos_tab, cos_tab], axis=-1), jnp.concatenate([-sin_tab, sin_tab], axis=-1)


def qkv_kernel(x_ref, g_ref, wq_ref, wk_ref, wv_ref, cos_ref, sin_ref, u_ref, send_ref):
    dests = send_ref.shape[0]
    kv_heads = wk_ref.shape[1] // HEAD_DIM
    repeat = dests // kv_heads
    x = x_ref[...].astype(jnp.float32)
    inv_rms = lax.rsqrt(jnp.mean(x * x, axis=-1, keepdims=True) + EPS)
    u_ref[...] = (x * inv_rms * g_ref[...]).astype(jnp.bfloat16)
    u = u_ref[...]
    cos, sin = cos_ref[...], sin_ref[...]

    def rotate(c):
        return (c * cos + pltpu.roll(c, HEAD_DIM // 2, 1) * sin).astype(jnp.bfloat16)

    q = jnp.dot(u, wq_ref[...], preferred_element_type=jnp.float32)
    for h in range(dests):
        send_ref[h, 0] = rotate(q[:, h * HEAD_DIM:(h + 1) * HEAD_DIM])
    k = jnp.dot(u, wk_ref[...], preferred_element_type=jnp.float32)
    v = jnp.dot(u, wv_ref[...], preferred_element_type=jnp.float32)
    for h in range(kv_heads):
        k_rot = rotate(k[:, h * HEAD_DIM:(h + 1) * HEAD_DIM])
        v_val = v[:, h * HEAD_DIM:(h + 1) * HEAD_DIM].astype(jnp.bfloat16)
        for r in range(repeat):
            send_ref[h * repeat + r, 1] = k_rot
            send_ref[h * repeat + r, 2] = v_val


def qkv_call(x_in, gain, w_q, w_k, w_v, cos, sin, dests):
    rows, width = x_in.shape
    tile = 256
    fixed = functools.partial(pl.BlockSpec, pipeline_mode=pl.Buffered(1))
    cols = w_q.shape[1] + w_k.shape[1] + w_v.shape[1]
    return pl.pallas_call(
        qkv_kernel,
        name="qkv_rope",
        grid=(rows // tile,),
        in_specs=[
            pl.BlockSpec((tile, width), lambda i: (i, 0)),
            fixed((1, width), lambda i: (0, 0)),
            fixed(w_q.shape, lambda i: (0, 0)),
            fixed(w_k.shape, lambda i: (0, 0)),
            fixed(w_v.shape, lambda i: (0, 0)),
            pl.BlockSpec((tile, HEAD_DIM), lambda i: (i, 0)),
            pl.BlockSpec((tile, HEAD_DIM), lambda i: (i, 0)),
        ],
        out_specs=[
            pl.BlockSpec((tile, width), lambda i: (i, 0)),
            pl.BlockSpec((dests, 3, tile, HEAD_DIM), lambda i: (0, 0, i, 0)),
        ],
        out_shape=[
            jax.ShapeDtypeStruct((rows, width), jnp.bfloat16),
            jax.ShapeDtypeStruct((dests, 3, rows, HEAD_DIM), jnp.bfloat16),
        ],
        compiler_params=pltpu.CompilerParams(vmem_limit_bytes=VMEM_LIMIT),
        cost_estimate=pl.CostEstimate(flops=2 * rows * width * cols, bytes_accessed=2 * (2 * rows * width + width * cols), transcendentals=0),
    )(x_in, gain, w_q, w_k, w_v, cos, sin)


def gate_up_kernel(u_ref, w1_ref, w3_ref, h_ref):
    u = u_ref[...]
    gate = jnp.dot(u, w1_ref[...], preferred_element_type=jnp.float32)
    up = jnp.dot(u, w3_ref[...], preferred_element_type=jnp.float32)
    h_ref[...] = (jax.nn.silu(gate) * up).astype(jnp.bfloat16)


def gate_up_call(u, w_gate, w_up):
    rows, width = u.shape
    cols = w_gate.shape[1]
    tile = 256
    return pl.pallas_call(
        gate_up_kernel,
        name="gate_up",
        grid=(cols // tile,),
        in_specs=[
            pl.BlockSpec((rows, width), lambda i: (0, 0), pipeline_mode=pl.Buffered(1)),
            pl.BlockSpec((width, tile), lambda i: (0, i)),
            pl.BlockSpec((width, tile), lambda i: (0, i)),
        ],
        out_specs=pl.BlockSpec((rows, tile), lambda i: (0, i)),
        out_shape=jax.ShapeDtypeStruct((rows, cols), jnp.bfloat16),
        compiler_params=pltpu.CompilerParams(vmem_limit_bytes=VMEM_LIMIT),
        cost_estimate=pl.CostEstimate(flops=4 * rows * width * cols, bytes_accessed=4 * width * cols + 2 * rows * (width + cols), transcendentals=rows * cols),
    )(u, w_gate, w_up)


def flash_kernel(q_ref, k_ref, v_ref, o_ref, s_buf, p_buf, alpha_buf, m_ref, l_ref, acc_ref, *, chunk, stride):
    src = pl.program_id(0)
    strips, strip_rows = q_ref.shape[2], q_ref.shape[3]
    rows = strips * strip_rows
    cols = k_ref.shape[2]
    q = q_ref[0, 0].reshape(rows, HEAD_DIM)

    def source_of(t):
        return jnp.where(t == 0, src, t - 1)

    def scores(t, slot):
        s_buf[slot] = lax.dot_general(q, k_ref[source_of(t), 0], (((1,), (1,)), ((), ())), preferred_element_type=jnp.float32)

    def soften(slot, masked):
        for r in range(0, rows, ROW_GROUP):
            group = pl.ds(r, ROW_GROUP)
            s = [s_buf[slot, group, pl.ds(g, HEAD_DIM)] for g in range(0, cols, HEAD_DIM)]
            if masked:
                row_id = lax.broadcasted_iota(jnp.int32, (ROW_GROUP, HEAD_DIM), 0) + (r // strip_rows * stride + chunk * strip_rows + r % strip_rows)
                col_id = lax.broadcasted_iota(jnp.int32, (ROW_GROUP, HEAD_DIM), 1)
                s = [jnp.where(col_id + g * HEAD_DIM <= row_id, s_g, -jnp.inf) for g, s_g in enumerate(s)]
            top = s[0]
            for s_g in s[1:]:
                top = jnp.maximum(top, s_g)
            top = jnp.broadcast_to(jnp.max(top, axis=1, keepdims=True), (ROW_GROUP, HEAD_DIM))
            if masked:
                alpha_buf[slot, group] = jnp.ones_like(top)
                total = jnp.zeros_like(top)
            else:
                m_old = m_ref[group]
                top = jnp.maximum(m_old, top)
                alpha = jnp.exp2((m_old - top) * EXP2_SCALE)
                alpha_buf[slot, group] = alpha
                total = l_ref[group] * alpha
            m_ref[group] = top
            for g, s_g in enumerate(s):
                p = jnp.exp2((s_g - top) * EXP2_SCALE)
                total = total + p
                p_buf[slot, group, pl.ds(g * HEAD_DIM, HEAD_DIM)] = p.astype(jnp.bfloat16)
            l_ref[group] = total

    def values(t, slot):
        acc_ref[...] = acc_ref[...] * alpha_buf[slot] + jnp.dot(p_buf[slot], v_ref[source_of(t), 0], preferred_element_type=jnp.float32)

    acc_ref[...] = jnp.zeros_like(acc_ref)
    scores(0, 0)
    scores(jnp.minimum(src, 1), 1)
    soften(0, True)

    def step(t, carry):
        for now in range(2):
            @pl.when(t % 2 == now)
            def _():
                scores(jnp.minimum(t + 1, src), 1 - now)
                soften(now, False)
                values(t - 1, 1 - now)
        return carry

    lax.fori_loop(1, src + 1, step, 0)
    for now in range(2):
        @pl.when(src % 2 == now)
        def _():
            values(src, now)
    o_ref[0] = (acc_ref[...] / jnp.sum(l_ref[...], axis=1, keepdims=True)).astype(jnp.bfloat16)


def flash_call(recv, chunk, strips, strip_rows):
    srcs, _, per_src, _ = recv.shape
    rows = strips * strip_rows
    work = srcs * rows * (srcs * per_src // 2)
    by_strip = recv.reshape(srcs, 3, strips, per_src // strips, HEAD_DIM)
    return pl.pallas_call(
        functools.partial(flash_kernel, chunk=chunk, stride=per_src // strips),
        name="flash",
        grid=(srcs,),
        in_specs=[
            pl.BlockSpec((1, 1, strips, strip_rows, HEAD_DIM), lambda s: (s, 0, 0, chunk, 0)),
            pl.BlockSpec((srcs, 1, per_src, HEAD_DIM), lambda s: (0, 1, 0, 0), pipeline_mode=pl.Buffered(1)),
            pl.BlockSpec((srcs, 1, per_src, HEAD_DIM), lambda s: (0, 2, 0, 0), pipeline_mode=pl.Buffered(1)),
        ],
        out_specs=pl.BlockSpec((1, rows, HEAD_DIM), lambda s: (s, 0, 0)),
        out_shape=jax.ShapeDtypeStruct((srcs, rows, HEAD_DIM), jnp.bfloat16),
        scratch_shapes=[
            pltpu.VMEM((2, rows, per_src), jnp.float32),
            pltpu.VMEM((2, rows, per_src), jnp.bfloat16),
            pltpu.VMEM((2, rows, HEAD_DIM), jnp.float32),
            pltpu.VMEM((rows, HEAD_DIM), jnp.float32),
            pltpu.VMEM((rows, HEAD_DIM), jnp.float32),
            pltpu.VMEM((rows, HEAD_DIM), jnp.float32),
        ],
        compiler_params=pltpu.CompilerParams(vmem_limit_bytes=VMEM_LIMIT),
        cost_estimate=pl.CostEstimate(flops=8 * work * HEAD_DIM, bytes_accessed=6 * srcs * per_src * HEAD_DIM, transcendentals=work),
    )(by_strip, recv, recv)


def down_out_kernel(h_ref, a_ref, wd_ref, wo_ref, o_ref):
    a = jnp.concatenate([a_ref[i] for i in range(a_ref.shape[0])], axis=1)
    attn = jnp.dot(a, wo_ref[...], preferred_element_type=jnp.float32)
    hidden = h_ref[...].reshape(a.shape[0], h_ref.shape[2])
    o_ref[...] = attn + jnp.dot(hidden, wd_ref[...], preferred_element_type=jnp.float32)


def down_out_call(hidden, a_heads, w_down, w_o, chunk, strips):
    heads, rows, _ = a_heads.shape
    ff, width = w_down.shape
    tile = 512
    depth = ff + w_o.shape[0]
    return pl.pallas_call(
        down_out_kernel,
        name="down_out",
        grid=(width // tile,),
        in_specs=[
            pl.BlockSpec((strips, rows // strips, ff), lambda i: (0, chunk, 0), pipeline_mode=pl.Buffered(1)),
            pl.BlockSpec((heads, rows, HEAD_DIM), lambda i: (0, 0, 0), pipeline_mode=pl.Buffered(1)),
            pl.BlockSpec((ff, tile), lambda i: (0, i)),
            pl.BlockSpec((w_o.shape[0], tile), lambda i: (0, i)),
        ],
        out_specs=pl.BlockSpec((rows, tile), lambda i: (0, i)),
        out_shape=jax.ShapeDtypeStruct((rows, width), jnp.float32),
        compiler_params=pltpu.CompilerParams(vmem_limit_bytes=VMEM_LIMIT),
        cost_estimate=pl.CostEstimate(flops=2 * rows * depth * width, bytes_accessed=2 * depth * width + 2 * rows * depth + 4 * rows * width, transcendentals=0),
    )(hidden.reshape(strips, hidden.shape[0] // strips, ff), a_heads, w_down, w_o)


def solution(mesh):
    sp_size = mesh.shape["sp"]
    tp_size = mesh.shape["tp"]
    row_spec = P(("rep", "sp"), None)
    cache_spec = P("rep", ("tp", "sp"), None)

    def layer_block(x_in, positions, norm_gain, w_q, w_k, w_v, w_o, w_gate, w_up, w_down):
        tok_local, width = x_in.shape
        cos, sin = rope_tables(positions)
        u, send = qkv_call(x_in, norm_gain[None, :], w_q, w_k, w_v, cos, sin, sp_size)
        recv = lax.all_to_all(send, "sp", 0, 0, tiled=True)
        hidden = gate_up_call(u, w_gate, w_up)
        recv, hidden = lax.optimization_barrier((recv, hidden))
        strip_rows = tok_local // (CHUNKS * tp_size)
        sums = []
        for c in range(CHUNKS):
            attn = flash_call(recv, c, tp_size, strip_rows)
            a_heads = lax.all_to_all(attn, "sp", 0, 0, tiled=True)
            partial = down_out_call(hidden, a_heads, w_down, w_o, c, tp_size)
            sums.append(lax.psum_scatter(partial, "tp", scatter_dimension=0, tiled=True))
        shard = tok_local // tp_size
        x_mine = lax.dynamic_slice_in_dim(x_in, lax.axis_index("tp") * shard, shard, axis=0)
        y_mine = (x_mine.astype(jnp.float32) + jnp.concatenate(sums, axis=0)).astype(jnp.bfloat16)
        y_out = lax.all_gather(y_mine, "tp", axis=0, tiled=True)
        k_all = recv[:, 1].reshape(sp_size * tok_local, 1, HEAD_DIM)
        v_all = recv[:, 2].reshape(sp_size * tok_local, 1, HEAD_DIM)
        return y_out, k_all, v_all

    return jax.shard_map(
        layer_block,
        mesh=mesh,
        in_specs=(row_spec, P(("rep", "sp")), P(None), P(None, "tp"), P(None, "tp"), P(None, "tp"), P("tp", None), P(None, "tp"), P(None, "tp"), P("tp", None)),
        out_specs=(row_spec, cache_spec, cache_spec),
        check_vma=False,
    )
```

```python
import functools
import math

import jax
import jax.numpy as jnp
from jax import lax
from jax.experimental import pallas as pl
from jax.experimental.pallas import tpu as pltpu
from jax.sharding import PartitionSpec as P

HEAD_DIM = 128
EPS = 1e-6
ROPE_BASE = 500000.0
SCORE_SCALE = HEAD_DIM ** -0.5
EXP2_SCALE = SCORE_SCALE * math.log2(math.e)
VMEM_LIMIT = 60 * 1024 * 1024
CHUNKS = 4
MESH = pl.DeviceIdType.MESH
ROW_GROUP = 32


def rope_tables(positions):
    inv_freq = ROPE_BASE ** (-(jnp.arange(HEAD_DIM // 2, dtype=jnp.float32) * (2.0 / HEAD_DIM)))
    angles = positions.astype(jnp.float32)[:, None] * inv_freq[None, :]
    cos_tab, sin_tab = jnp.cos(angles), jnp.sin(angles)
    return jnp.concatenate([cos_tab, cos_tab], axis=-1), jnp.concatenate([-sin_tab, sin_tab], axis=-1)


def qkv_kernel(x_ref, g_ref, wq_ref, wk_ref, wv_ref, cos_ref, sin_ref, u_ref, send_ref):
    dests = send_ref.shape[0]
    kv_heads = wk_ref.shape[1] // HEAD_DIM
    repeat = dests // kv_heads
    x = x_ref[...].astype(jnp.float32)
    inv_rms = lax.rsqrt(jnp.mean(x * x, axis=-1, keepdims=True) + EPS)
    u_ref[...] = (x * inv_rms * g_ref[...]).astype(jnp.bfloat16)
    u = u_ref[...]
    cos, sin = cos_ref[...], sin_ref[...]

    def rotate(c):
        return (c * cos + pltpu.roll(c, HEAD_DIM // 2, 1) * sin).astype(jnp.bfloat16)

    q = jnp.dot(u, wq_ref[...], preferred_element_type=jnp.float32)
    for h in range(dests):
        send_ref[h, 0] = rotate(q[:, h * HEAD_DIM:(h + 1) * HEAD_DIM])
    k = jnp.dot(u, wk_ref[...], preferred_element_type=jnp.float32)
    v = jnp.dot(u, wv_ref[...], preferred_element_type=jnp.float32)
    for h in range(kv_heads):
        k_rot = rotate(k[:, h * HEAD_DIM:(h + 1) * HEAD_DIM])
        v_val = v[:, h * HEAD_DIM:(h + 1) * HEAD_DIM].astype(jnp.bfloat16)
        for r in range(repeat):
            send_ref[h * repeat + r, 1] = k_rot
            send_ref[h * repeat + r, 2] = v_val


def qkv_call(x_in, gain, w_q, w_k, w_v, cos, sin, dests):
    rows, width = x_in.shape
    tile = 256
    fixed = functools.partial(pl.BlockSpec, pipeline_mode=pl.Buffered(1))
    cols = w_q.shape[1] + w_k.shape[1] + w_v.shape[1]
    return pl.pallas_call(
        qkv_kernel,
        name="qkv_rope",
        grid=(rows // tile,),
        in_specs=[
            pl.BlockSpec((tile, width), lambda i: (i, 0)),
            fixed((1, width), lambda i: (0, 0)),
            fixed(w_q.shape, lambda i: (0, 0)),
            fixed(w_k.shape, lambda i: (0, 0)),
            fixed(w_v.shape, lambda i: (0, 0)),
            pl.BlockSpec((tile, HEAD_DIM), lambda i: (i, 0)),
            pl.BlockSpec((tile, HEAD_DIM), lambda i: (i, 0)),
        ],
        out_specs=[
            pl.BlockSpec((tile, width), lambda i: (i, 0)),
            pl.BlockSpec((dests, 3, tile, HEAD_DIM), lambda i: (0, 0, i, 0)),
        ],
        out_shape=[
            jax.ShapeDtypeStruct((rows, width), jnp.bfloat16),
            jax.ShapeDtypeStruct((dests, 3, rows, HEAD_DIM), jnp.bfloat16),
        ],
        compiler_params=pltpu.CompilerParams(vmem_limit_bytes=VMEM_LIMIT),
        cost_estimate=pl.CostEstimate(flops=2 * rows * width * cols, bytes_accessed=2 * (2 * rows * width + width * cols), transcendentals=0),
    )(x_in, gain, w_q, w_k, w_v, cos, sin)


def gate_up_kernel(u_ref, w1_ref, w3_ref, h_ref):
    u = u_ref[...]
    gate = jnp.dot(u, w1_ref[...], preferred_element_type=jnp.float32)
    up = jnp.dot(u, w3_ref[...], preferred_element_type=jnp.float32)
    h_ref[...] = (jax.nn.silu(gate) * up).astype(jnp.bfloat16)


def gate_up_call(u, w_gate, w_up):
    rows, width = u.shape
    cols = w_gate.shape[1]
    tile = 256
    return pl.pallas_call(
        gate_up_kernel,
        name="gate_up",
        grid=(cols // tile,),
        in_specs=[
            pl.BlockSpec((rows, width), lambda i: (0, 0), pipeline_mode=pl.Buffered(1)),
            pl.BlockSpec((width, tile), lambda i: (0, i)),
            pl.BlockSpec((width, tile), lambda i: (0, i)),
        ],
        out_specs=pl.BlockSpec((rows, tile), lambda i: (0, i)),
        out_shape=jax.ShapeDtypeStruct((rows, cols), jnp.bfloat16),
        compiler_params=pltpu.CompilerParams(vmem_limit_bytes=VMEM_LIMIT),
        cost_estimate=pl.CostEstimate(flops=4 * rows * width * cols, bytes_accessed=4 * width * cols + 2 * rows * (width + cols), transcendentals=rows * cols),
    )(u, w_gate, w_up)


def flash_kernel(q_ref, k_ref, v_ref, out_ref, tiles, s_buf, p_buf, alpha_buf, m_ref, l_ref, acc_ref, send_sem, recv_sem, own_sem, *, chunk, stride):
    srcs = k_ref.shape[0]
    here = pl.program_id(0)
    src = srcs - 1 - here
    me = lax.axis_index("sp")

    def to_peer(dest):
        return pltpu.make_async_remote_copy(
            src_ref=tiles.at[dest], dst_ref=out_ref.at[me], send_sem=send_sem.at[dest], recv_sem=recv_sem.at[me],
            device_id={"sp": dest}, device_id_type=MESH)

    def to_self():
        return pltpu.make_async_copy(tiles.at[me], out_ref.at[me], own_sem)

    def send(dest):
        @pl.when(dest == me)
        def _():
            to_self().start()

        @pl.when(dest != me)
        def _():
            to_peer(dest).start()

    @pl.when(here == 0)
    def _():
        barrier = pltpu.get_barrier_semaphore()
        for j in range(1, srcs):
            pl.semaphore_signal(barrier, inc=1, device_id={"sp": lax.rem(me + j, srcs)}, device_id_type=MESH)
        pl.semaphore_wait(barrier, srcs - 1)

    @pl.when(here > 0)
    def _():
        send(src + 1)

    strips, strip_rows = q_ref.shape[2], q_ref.shape[3]
    rows = strips * strip_rows
    cols = k_ref.shape[2]
    q = q_ref[0, 0].reshape(rows, HEAD_DIM)

    def source_of(t):
        return jnp.where(t == 0, src, t - 1)

    def scores(t, slot):
        s_buf[slot] = lax.dot_general(q, k_ref[source_of(t), 0], (((1,), (1,)), ((), ())), preferred_element_type=jnp.float32)

    def soften(slot, masked):
        for r in range(0, rows, ROW_GROUP):
            group = pl.ds(r, ROW_GROUP)
            s = [s_buf[slot, group, pl.ds(g, HEAD_DIM)] for g in range(0, cols, HEAD_DIM)]
            if masked:
                row_id = lax.broadcasted_iota(jnp.int32, (ROW_GROUP, HEAD_DIM), 0) + (r // strip_rows * stride + chunk * strip_rows + r % strip_rows)
                col_id = lax.broadcasted_iota(jnp.int32, (ROW_GROUP, HEAD_DIM), 1)
                s = [jnp.where(col_id + g * HEAD_DIM <= row_id, s_g, -jnp.inf) for g, s_g in enumerate(s)]
            top = s[0]
            for s_g in s[1:]:
                top = jnp.maximum(top, s_g)
            top = jnp.broadcast_to(jnp.max(top, axis=1, keepdims=True), (ROW_GROUP, HEAD_DIM))
            if masked:
                alpha_buf[slot, group] = jnp.ones_like(top)
                total = jnp.zeros_like(top)
            else:
                m_old = m_ref[group]
                top = jnp.maximum(m_old, top)
                alpha = jnp.exp2((m_old - top) * EXP2_SCALE)
                alpha_buf[slot, group] = alpha
                total = l_ref[group] * alpha
            m_ref[group] = top
            for g, s_g in enumerate(s):
                p = jnp.exp2((s_g - top) * EXP2_SCALE)
                total = total + p
                p_buf[slot, group, pl.ds(g * HEAD_DIM, HEAD_DIM)] = p.astype(jnp.bfloat16)
            l_ref[group] = total

    def values(t, slot):
        acc_ref[...] = acc_ref[...] * alpha_buf[slot] + jnp.dot(p_buf[slot], v_ref[source_of(t), 0], preferred_element_type=jnp.float32)

    acc_ref[...] = jnp.zeros_like(acc_ref)
    scores(0, 0)
    scores(jnp.minimum(src, 1), 1)
    soften(0, True)

    def step(t, carry):
        for now in range(2):
            @pl.when(t % 2 == now)
            def _():
                scores(jnp.minimum(t + 1, src), 1 - now)
                soften(now, False)
                values(t - 1, 1 - now)
        return carry

    lax.fori_loop(1, src + 1, step, 0)
    for now in range(2):
        @pl.when(src % 2 == now)
        def _():
            values(src, now)
    tiles[src] = (acc_ref[...] / jnp.sum(l_ref[...], axis=1, keepdims=True)).astype(jnp.bfloat16)

    @pl.when(here == srcs - 1)
    def _():
        for dest in range(1, srcs):
            @pl.when(dest != me)
            def _():
                to_peer(dest).wait_send()
        send(0)

        @pl.when(me != 0)
        def _():
            to_peer(0).wait_send()
        to_self().wait()
        for j in range(1, srcs):
            peer = lax.rem(me + j, srcs)
            pltpu.make_async_remote_copy(
                src_ref=tiles.at[0], dst_ref=out_ref.at[peer], send_sem=send_sem.at[0], recv_sem=recv_sem.at[peer],
                device_id={"sp": peer}, device_id_type=MESH).wait_recv()


def flash_call(recv, chunk, strips, strip_rows):
    srcs, _, per_src, _ = recv.shape
    rows = strips * strip_rows
    work = srcs * rows * (srcs * per_src // 2)
    by_strip = recv.reshape(srcs, 3, strips, per_src // strips, HEAD_DIM)
    return pl.pallas_call(
        functools.partial(flash_kernel, chunk=chunk, stride=per_src // strips),
        name="flash",
        grid=(srcs,),
        in_specs=[
            pl.BlockSpec((1, 1, strips, strip_rows, HEAD_DIM), lambda s: (srcs - 1 - s, 0, 0, chunk, 0)),
            pl.BlockSpec((srcs, 1, per_src, HEAD_DIM), lambda s: (0, 1, 0, 0), pipeline_mode=pl.Buffered(1)),
            pl.BlockSpec((srcs, 1, per_src, HEAD_DIM), lambda s: (0, 2, 0, 0), pipeline_mode=pl.Buffered(1)),
        ],
        out_specs=pl.BlockSpec(memory_space=pl.ANY),
        out_shape=jax.ShapeDtypeStruct((srcs, rows, HEAD_DIM), jnp.bfloat16),
        scratch_shapes=[
            pltpu.VMEM((srcs, rows, HEAD_DIM), jnp.bfloat16),
            pltpu.VMEM((2, rows, per_src), jnp.float32),
            pltpu.VMEM((2, rows, per_src), jnp.bfloat16),
            pltpu.VMEM((2, rows, HEAD_DIM), jnp.float32),
            pltpu.VMEM((rows, HEAD_DIM), jnp.float32),
            pltpu.VMEM((rows, HEAD_DIM), jnp.float32),
            pltpu.VMEM((rows, HEAD_DIM), jnp.float32),
            pltpu.SemaphoreType.DMA((srcs,)),
            pltpu.SemaphoreType.DMA((srcs,)),
            pltpu.SemaphoreType.DMA,
        ],
        compiler_params=pltpu.CompilerParams(vmem_limit_bytes=VMEM_LIMIT, collective_id=chunk, has_side_effects=True),
        cost_estimate=pl.CostEstimate(flops=8 * work * HEAD_DIM, bytes_accessed=6 * srcs * per_src * HEAD_DIM, transcendentals=work),
    )(by_strip, recv, recv)


def down_out_kernel(h_ref, a_ref, wd_ref, wo_ref, o_ref):
    a = jnp.concatenate([a_ref[i] for i in range(a_ref.shape[0])], axis=1)
    attn = jnp.dot(a, wo_ref[...], preferred_element_type=jnp.float32)
    hidden = h_ref[...].reshape(a.shape[0], h_ref.shape[2])
    o_ref[...] = attn + jnp.dot(hidden, wd_ref[...], preferred_element_type=jnp.float32)


def down_out_call(hidden, a_heads, w_down, w_o, chunk, strips):
    heads, rows, _ = a_heads.shape
    ff, width = w_down.shape
    tile = 512
    depth = ff + w_o.shape[0]
    return pl.pallas_call(
        down_out_kernel,
        name="down_out",
        grid=(width // tile,),
        in_specs=[
            pl.BlockSpec((strips, rows // strips, ff), lambda i: (0, chunk, 0), pipeline_mode=pl.Buffered(1)),
            pl.BlockSpec((heads, rows, HEAD_DIM), lambda i: (0, 0, 0), pipeline_mode=pl.Buffered(1)),
            pl.BlockSpec((ff, tile), lambda i: (0, i)),
            pl.BlockSpec((w_o.shape[0], tile), lambda i: (0, i)),
        ],
        out_specs=pl.BlockSpec((rows, tile), lambda i: (0, i)),
        out_shape=jax.ShapeDtypeStruct((rows, width), jnp.float32),
        compiler_params=pltpu.CompilerParams(vmem_limit_bytes=VMEM_LIMIT),
        cost_estimate=pl.CostEstimate(flops=2 * rows * depth * width, bytes_accessed=2 * depth * width + 2 * rows * depth + 4 * rows * width, transcendentals=0),
    )(hidden.reshape(strips, hidden.shape[0] // strips, ff), a_heads, w_down, w_o)


def gather_kernel(*refs, pieces, n, base):
    own, out_ref = refs[:pieces], refs[pieces]
    send_sem, recv_sem, own_sem = refs[pieces + 1:]
    me = lax.axis_index("tp")
    right, left = lax.rem(me + 1, n), lax.rem(me + n - 1, n)
    half = own[0].shape[0] // 2
    barrier = pltpu.get_barrier_semaphore()
    for peer in (left, right):
        pl.semaphore_signal(barrier, inc=1, device_id={"tp": peer}, device_id_type=MESH)
    pl.semaphore_wait(barrier, 2)

    def hop(h, i, way):
        peer = right if way == 0 else left
        owner = lax.rem(me + (n - h if way == 0 else h), n)
        rows = pl.ds(way * half, half)
        place = out_ref.at[owner, base + i, rows]
        return pltpu.make_async_remote_copy(
            src_ref=own[i].at[rows] if h == 0 else place, dst_ref=place,
            send_sem=send_sem.at[way, h, i], recv_sem=recv_sem.at[way, h, i],
            device_id={"tp": peer}, device_id_type=MESH)

    for i in range(pieces):
        for way in range(2):
            hop(0, i, way).start()
    for i in range(pieces):
        pltpu.make_async_copy(own[i], out_ref.at[me, base + i], own_sem.at[i]).start()
    for h in range(1, n):
        for i in range(pieces):
            for way in range(2):
                hop(h - 1, i, way).wait_recv()
                if h < n - 1:
                    hop(h, i, way).start()
    for h in range(n - 1):
        for i in range(pieces):
            for way in range(2):
                hop(h, i, way).wait_send()
    for i in range(pieces):
        pltpu.make_async_copy(own[i], out_ref.at[me, base + i], own_sem.at[i]).wait()


def gather_call(own, n, slots, base, collective_id):
    rows, width = own[0].shape
    pieces = len(own)
    moved = 2 * (n - 1) * pieces * rows * width
    return pl.pallas_call(
        functools.partial(gather_kernel, pieces=pieces, n=n, base=base),
        name="gather_tp",
        in_specs=[pl.BlockSpec(memory_space=pltpu.VMEM)] * pieces,
        out_specs=pl.BlockSpec(memory_space=pl.ANY),
        out_shape=jax.ShapeDtypeStruct((n, slots, rows, width), jnp.bfloat16),
        scratch_shapes=[
            pltpu.SemaphoreType.DMA((2, n - 1, pieces)),
            pltpu.SemaphoreType.DMA((2, n - 1, pieces)),
            pltpu.SemaphoreType.DMA((pieces,)),
        ],
        compiler_params=pltpu.CompilerParams(vmem_limit_bytes=VMEM_LIMIT, collective_id=collective_id, has_side_effects=True),
        cost_estimate=pl.CostEstimate(flops=moved * 1000, bytes_accessed=moved, transcendentals=0),
    )(*own)


def solution(mesh):
    sp_size = mesh.shape["sp"]
    tp_size = mesh.shape["tp"]
    row_spec = P(("rep", "sp"), None)
    cache_spec = P("rep", ("tp", "sp"), None)

    def layer_block(x_in, positions, norm_gain, w_q, w_k, w_v, w_o, w_gate, w_up, w_down):
        tok_local, width = x_in.shape
        cos, sin = rope_tables(positions)
        u, send = qkv_call(x_in, norm_gain[None, :], w_q, w_k, w_v, cos, sin, sp_size)
        recv = lax.all_to_all(send, "sp", 0, 0, tiled=True)
        hidden = gate_up_call(u, w_gate, w_up)
        recv, hidden = lax.optimization_barrier((recv, hidden))
        strip_rows = tok_local // (CHUNKS * tp_size)
        shard = tok_local // tp_size
        x_mine = lax.dynamic_slice_in_dim(x_in, lax.axis_index("tp") * shard, shard, axis=0)
        sums = []
        for c in range(CHUNKS):
            a_heads = flash_call(recv, c, tp_size, strip_rows)
            partial = down_out_call(hidden, a_heads, w_down, w_o, c, tp_size)
            sums.append(lax.psum_scatter(partial, "tp", scatter_dimension=0, tiled=True))

        def finish(c, x_rows, total):
            return (x_rows[c * strip_rows:(c + 1) * strip_rows].astype(jnp.float32) + total).astype(jnp.bfloat16)

        y_early, _ = lax.optimization_barrier(([finish(c, x_mine, sums[c]) for c in range(CHUNKS - 1)], partial))
        early = gather_call(y_early, tp_size, CHUNKS - 1, 0, CHUNKS)
        x_late, early = lax.optimization_barrier((x_mine, early))
        last = gather_call([finish(CHUNKS - 1, x_late, sums[-1])], tp_size, 1, 0, CHUNKS + 1)
        y_out = jnp.concatenate([early, last], axis=1).reshape(tok_local, width)
        k_all = recv[:, 1].reshape(sp_size * tok_local, 1, HEAD_DIM)
        v_all = recv[:, 2].reshape(sp_size * tok_local, 1, HEAD_DIM)
        return y_out, k_all, v_all

    return jax.shard_map(
        layer_block,
        mesh=mesh,
        in_specs=(row_spec, P(("rep", "sp")), P(None), P(None, "tp"), P(None, "tp"), P(None, "tp"), P("tp", None), P(None, "tp"), P(None, "tp"), P("tp", None)),
        out_specs=(row_spec, cache_spec, cache_spec),
        check_vma=False,
    )
```

```python
import functools
import math

import jax
import jax.numpy as jnp
from jax import lax
from jax.experimental import pallas as pl
from jax.experimental.pallas import tpu as pltpu
from jax.sharding import PartitionSpec as P

HEAD_DIM = 128
EPS = 1e-6
ROPE_BASE = 500000.0
SCORE_SCALE = HEAD_DIM ** -0.5
EXP2_SCALE = SCORE_SCALE * math.log2(math.e)
VMEM_LIMIT = 60 * 1024 * 1024
CHUNKS = 4
LAG = 2
MESH = pl.DeviceIdType.MESH
ROW_GROUP = 32


def rope_tables(positions):
    inv_freq = ROPE_BASE ** (-(jnp.arange(HEAD_DIM // 2, dtype=jnp.float32) * (2.0 / HEAD_DIM)))
    angles = positions.astype(jnp.float32)[:, None] * inv_freq[None, :]
    cos_tab, sin_tab = jnp.cos(angles), jnp.sin(angles)
    return jnp.concatenate([cos_tab, cos_tab], axis=-1), jnp.concatenate([-sin_tab, sin_tab], axis=-1)


def qkv_kernel(x_ref, g_ref, wq_ref, wk_ref, wv_ref, cos_ref, sin_ref, u_ref, send_ref):
    dests = send_ref.shape[0]
    kv_heads = wk_ref.shape[1] // HEAD_DIM
    repeat = dests // kv_heads
    x = x_ref[...].astype(jnp.float32)
    inv_rms = lax.rsqrt(jnp.mean(x * x, axis=-1, keepdims=True) + EPS)
    u_ref[...] = (x * inv_rms * g_ref[...]).astype(jnp.bfloat16)
    u = u_ref[...]
    cos, sin = cos_ref[...], sin_ref[...]

    def rotate(c):
        return (c * cos + pltpu.roll(c, HEAD_DIM // 2, 1) * sin).astype(jnp.bfloat16)

    q = jnp.dot(u, wq_ref[...], preferred_element_type=jnp.float32)
    for h in range(dests):
        send_ref[h, 0] = rotate(q[:, h * HEAD_DIM:(h + 1) * HEAD_DIM])
    k = jnp.dot(u, wk_ref[...], preferred_element_type=jnp.float32)
    v = jnp.dot(u, wv_ref[...], preferred_element_type=jnp.float32)
    for h in range(kv_heads):
        k_rot = rotate(k[:, h * HEAD_DIM:(h + 1) * HEAD_DIM])
        v_val = v[:, h * HEAD_DIM:(h + 1) * HEAD_DIM].astype(jnp.bfloat16)
        for r in range(repeat):
            send_ref[h * repeat + r, 1] = k_rot
            send_ref[h * repeat + r, 2] = v_val


def qkv_call(x_in, gain, w_q, w_k, w_v, cos, sin, dests):
    rows, width = x_in.shape
    tile = 256
    fixed = functools.partial(pl.BlockSpec, pipeline_mode=pl.Buffered(1))
    cols = w_q.shape[1] + w_k.shape[1] + w_v.shape[1]
    return pl.pallas_call(
        qkv_kernel,
        name="qkv_rope",
        grid=(rows // tile,),
        in_specs=[
            pl.BlockSpec((tile, width), lambda i: (i, 0)),
            fixed((1, width), lambda i: (0, 0)),
            fixed(w_q.shape, lambda i: (0, 0)),
            fixed(w_k.shape, lambda i: (0, 0)),
            fixed(w_v.shape, lambda i: (0, 0)),
            pl.BlockSpec((tile, HEAD_DIM), lambda i: (i, 0)),
            pl.BlockSpec((tile, HEAD_DIM), lambda i: (i, 0)),
        ],
        out_specs=[
            pl.BlockSpec((tile, width), lambda i: (i, 0)),
            pl.BlockSpec((dests, 3, tile, HEAD_DIM), lambda i: (0, 0, i, 0)),
        ],
        out_shape=[
            jax.ShapeDtypeStruct((rows, width), jnp.bfloat16),
            jax.ShapeDtypeStruct((dests, 3, rows, HEAD_DIM), jnp.bfloat16),
        ],
        compiler_params=pltpu.CompilerParams(vmem_limit_bytes=VMEM_LIMIT),
        cost_estimate=pl.CostEstimate(flops=2 * rows * width * cols, bytes_accessed=2 * (2 * rows * width + width * cols), transcendentals=0),
    )(x_in, gain, w_q, w_k, w_v, cos, sin)


def gate_up_kernel(u_ref, w1_ref, w3_ref, h_ref):
    u = u_ref[...]
    gate = jnp.dot(u, w1_ref[...], preferred_element_type=jnp.float32)
    up = jnp.dot(u, w3_ref[...], preferred_element_type=jnp.float32)
    h_ref[...] = (jax.nn.silu(gate) * up).astype(jnp.bfloat16)


def gate_up_call(u, w_gate, w_up):
    rows, width = u.shape
    cols = w_gate.shape[1]
    tile = 256
    return pl.pallas_call(
        gate_up_kernel,
        name="gate_up",
        grid=(cols // tile,),
        in_specs=[
            pl.BlockSpec((rows, width), lambda i: (0, 0), pipeline_mode=pl.Buffered(1)),
            pl.BlockSpec((width, tile), lambda i: (0, i)),
            pl.BlockSpec((width, tile), lambda i: (0, i)),
        ],
        out_specs=pl.BlockSpec((rows, tile), lambda i: (0, i)),
        out_shape=jax.ShapeDtypeStruct((rows, cols), jnp.bfloat16),
        compiler_params=pltpu.CompilerParams(vmem_limit_bytes=VMEM_LIMIT),
        cost_estimate=pl.CostEstimate(flops=4 * rows * width * cols, bytes_accessed=4 * width * cols + 2 * rows * (width + cols), transcendentals=rows * cols),
    )(u, w_gate, w_up)


def flash_kernel(q_ref, k_ref, v_ref, out_ref, tiles, s_buf, p_buf, alpha_buf, m_ref, l_ref, acc_ref, send_sem, recv_sem, own_sem, *, chunk, stride):
    srcs = k_ref.shape[0]
    here = pl.program_id(0)
    me = lax.axis_index("sp")
    src = lax.rem(me + 1 + here, srcs)

    def to_peer(dest):
        return pltpu.make_async_remote_copy(
            src_ref=tiles.at[dest], dst_ref=out_ref.at[me], send_sem=send_sem.at[dest], recv_sem=recv_sem.at[me],
            device_id={"sp": dest}, device_id_type=MESH)

    def to_self():
        return pltpu.make_async_copy(tiles.at[me], out_ref.at[me], own_sem)

    @pl.when(here == 0)
    def _():
        barrier = pltpu.get_barrier_semaphore()
        for j in range(1, srcs):
            pl.semaphore_signal(barrier, inc=1, device_id={"sp": lax.rem(me + j, srcs)}, device_id_type=MESH)
        pl.semaphore_wait(barrier, srcs - 1)

    @pl.when(here > 0)
    def _():
        to_peer(lax.rem(me + here, srcs)).start()

    strips, strip_rows = q_ref.shape[2], q_ref.shape[3]
    rows = strips * strip_rows
    cols = k_ref.shape[2]
    q = q_ref[src, 0].reshape(rows, HEAD_DIM)

    def source_of(t):
        return jnp.where(t == 0, src, t - 1)

    def scores(t, slot):
        s_buf[slot] = lax.dot_general(q, k_ref[source_of(t), 0], (((1,), (1,)), ((), ())), preferred_element_type=jnp.float32)

    def soften(slot, masked):
        for r in range(0, rows, ROW_GROUP):
            group = pl.ds(r, ROW_GROUP)
            s = [s_buf[slot, group, pl.ds(g, HEAD_DIM)] for g in range(0, cols, HEAD_DIM)]
            if masked:
                row_id = lax.broadcasted_iota(jnp.int32, (ROW_GROUP, HEAD_DIM), 0) + (r // strip_rows * stride + chunk * strip_rows + r % strip_rows)
                col_id = lax.broadcasted_iota(jnp.int32, (ROW_GROUP, HEAD_DIM), 1)
                s = [jnp.where(col_id + g * HEAD_DIM <= row_id, s_g, -jnp.inf) for g, s_g in enumerate(s)]
            top = s[0]
            for s_g in s[1:]:
                top = jnp.maximum(top, s_g)
            top = jnp.broadcast_to(jnp.max(top, axis=1, keepdims=True), (ROW_GROUP, HEAD_DIM))
            if masked:
                alpha_buf[slot, group] = jnp.ones_like(top)
                total = jnp.zeros_like(top)
            else:
                m_old = m_ref[group]
                top = jnp.maximum(m_old, top)
                alpha = jnp.exp2((m_old - top) * EXP2_SCALE)
                alpha_buf[slot, group] = alpha
                total = l_ref[group] * alpha
            m_ref[group] = top
            for g, s_g in enumerate(s):
                p = jnp.exp2((s_g - top) * EXP2_SCALE)
                total = total + p
                p_buf[slot, group, pl.ds(g * HEAD_DIM, HEAD_DIM)] = p.astype(jnp.bfloat16)
            l_ref[group] = total

    def values(t, slot):
        acc_ref[...] = acc_ref[...] * alpha_buf[slot] + jnp.dot(p_buf[slot], v_ref[source_of(t), 0], preferred_element_type=jnp.float32)

    acc_ref[...] = jnp.zeros_like(acc_ref)
    scores(0, 0)
    scores(jnp.minimum(src, 1), 1)
    soften(0, True)

    def step(t, carry):
        for now in range(2):
            @pl.when(t % 2 == now)
            def _():
                scores(jnp.minimum(t + 1, src), 1 - now)
                soften(now, False)
                values(t - 1, 1 - now)
        return carry

    lax.fori_loop(1, src + 1, step, 0)
    for now in range(2):
        @pl.when(src % 2 == now)
        def _():
            values(src, now)
    tiles[src] = (acc_ref[...] / jnp.sum(l_ref[...], axis=1, keepdims=True)).astype(jnp.bfloat16)

    @pl.when(here == srcs - 1)
    def _():
        to_self().start()
        for j in range(1, srcs):
            to_peer(lax.rem(me + j, srcs)).wait_send()
        to_self().wait()
        for j in range(1, srcs):
            peer = lax.rem(me + j, srcs)
            pltpu.make_async_remote_copy(
                src_ref=tiles.at[0], dst_ref=out_ref.at[peer], send_sem=send_sem.at[0], recv_sem=recv_sem.at[peer],
                device_id={"sp": peer}, device_id_type=MESH).wait_recv()


def flash_call(recv, chunk, strips, strip_rows):
    srcs, _, per_src, _ = recv.shape
    rows = strips * strip_rows
    work = srcs * rows * (srcs * per_src // 2)
    by_strip = recv.reshape(srcs, 3, strips, per_src // strips, HEAD_DIM)
    return pl.pallas_call(
        functools.partial(flash_kernel, chunk=chunk, stride=per_src // strips),
        name="flash",
        grid=(srcs,),
        in_specs=[
            pl.BlockSpec((srcs, 1, strips, strip_rows, HEAD_DIM), lambda s: (0, 0, 0, chunk, 0), pipeline_mode=pl.Buffered(1)),
            pl.BlockSpec((srcs, 1, per_src, HEAD_DIM), lambda s: (0, 1, 0, 0), pipeline_mode=pl.Buffered(1)),
            pl.BlockSpec((srcs, 1, per_src, HEAD_DIM), lambda s: (0, 2, 0, 0), pipeline_mode=pl.Buffered(1)),
        ],
        out_specs=pl.BlockSpec(memory_space=pl.ANY),
        out_shape=jax.ShapeDtypeStruct((srcs, rows, HEAD_DIM), jnp.bfloat16),
        scratch_shapes=[
            pltpu.VMEM((srcs, rows, HEAD_DIM), jnp.bfloat16),
            pltpu.VMEM((2, rows, per_src), jnp.float32),
            pltpu.VMEM((2, rows, per_src), jnp.bfloat16),
            pltpu.VMEM((2, rows, HEAD_DIM), jnp.float32),
            pltpu.VMEM((rows, HEAD_DIM), jnp.float32),
            pltpu.VMEM((rows, HEAD_DIM), jnp.float32),
            pltpu.VMEM((rows, HEAD_DIM), jnp.float32),
            pltpu.SemaphoreType.DMA((srcs,)),
            pltpu.SemaphoreType.DMA((srcs,)),
            pltpu.SemaphoreType.DMA,
        ],
        compiler_params=pltpu.CompilerParams(vmem_limit_bytes=VMEM_LIMIT, collective_id=chunk, has_side_effects=True),
        cost_estimate=pl.CostEstimate(flops=8 * work * HEAD_DIM, bytes_accessed=6 * srcs * per_src * HEAD_DIM, transcendentals=work),
    )(by_strip, recv, recv)


def ring_hops(own, out_ref, send_sem, recv_sem, n, base):
    me = lax.axis_index("tp")
    right, left = lax.rem(me + 1, n), lax.rem(me + n - 1, n)
    half = own[0].shape[0] // 2

    def meet():
        barrier = pltpu.get_barrier_semaphore()
        for peer in (left, right):
            pl.semaphore_signal(barrier, inc=1, device_id={"tp": peer}, device_id_type=MESH)
        pl.semaphore_wait(barrier, 2)

    def hop(h, i, way):
        owner = lax.rem(me + (n - h if way == 0 else h), n)
        rows = pl.ds(way * half, half)
        place = out_ref.at[owner, base + i, rows]
        return pltpu.make_async_remote_copy(
            src_ref=own[i].at[rows] if h == 0 else place, dst_ref=place,
            send_sem=send_sem.at[way, h, i], recv_sem=recv_sem.at[way, h, i],
            device_id={"tp": right if way == 0 else left}, device_id_type=MESH)

    return me, meet, hop


def down_out_kernel(*refs, n):
    h_ref, a_ref, wd_ref, wo_ref = refs[:4]
    step, last = pl.program_id(0), pl.num_programs(0) - 1
    if n:
        own, o_ref, gathered, send_sem, recv_sem, own_sem = refs[4:]
        me, meet, hop = ring_hops([own], gathered, send_sem, recv_sem, n, 0)

        def keep():
            return pltpu.make_async_copy(own, gathered.at[me, 0], own_sem)

        @pl.when(step == 0)
        def _():
            meet()
            for way in range(2):
                hop(0, 0, way).start()
            keep().start()

        for h in range(1, n - 1):
            @pl.when(step == jnp.minimum(1 + 2 * h, last))
            def _():
                for way in range(2):
                    hop(h - 1, 0, way).wait_recv()
                    hop(h, 0, way).start()
    else:
        o_ref, = refs[4:]
    a = jnp.concatenate([a_ref[i] for i in range(a_ref.shape[0])], axis=1)
    attn = jnp.dot(a, wo_ref[...], preferred_element_type=jnp.float32)
    hidden = h_ref[...].reshape(a.shape[0], h_ref.shape[2])
    o_ref[...] = attn + jnp.dot(hidden, wd_ref[...], preferred_element_type=jnp.float32)
    if n:
        @pl.when(step == last)
        def _():
            for way in range(2):
                hop(n - 2, 0, way).wait_recv()
                for h in range(n - 1):
                    hop(h, 0, way).wait_send()
            keep().wait()


def down_out_call(hidden, a_heads, w_down, w_o, chunk, strips, own=None, collective_id=None):
    heads, rows, _ = a_heads.shape
    ff, width = w_down.shape
    tile = 512
    depth = ff + w_o.shape[0]
    in_specs = [
        pl.BlockSpec((strips, rows // strips, ff), lambda i: (0, chunk, 0), pipeline_mode=pl.Buffered(1)),
        pl.BlockSpec((heads, rows, HEAD_DIM), lambda i: (0, 0, 0), pipeline_mode=pl.Buffered(1)),
        pl.BlockSpec((ff, tile), lambda i: (0, i)),
        pl.BlockSpec((w_o.shape[0], tile), lambda i: (0, i)),
    ]
    out_specs = [pl.BlockSpec((rows, tile), lambda i: (0, i))]
    out_shape = [jax.ShapeDtypeStruct((rows, width), jnp.float32)]
    operands = [hidden.reshape(strips, hidden.shape[0] // strips, ff), a_heads, w_down, w_o]
    scratch, n, params = [], 0, {}
    if own is not None:
        n = strips
        in_specs.append(pl.BlockSpec(own.shape, lambda i: (0, 0), pipeline_mode=pl.Buffered(1)))
        out_specs.append(pl.BlockSpec(memory_space=pl.ANY))
        out_shape.append(jax.ShapeDtypeStruct((n, 1, *own.shape), own.dtype))
        operands.append(own)
        scratch = [pltpu.SemaphoreType.DMA((2, n - 1, 1)), pltpu.SemaphoreType.DMA((2, n - 1, 1)), pltpu.SemaphoreType.DMA]
        params = {"collective_id": collective_id, "has_side_effects": True}
    return pl.pallas_call(
        functools.partial(down_out_kernel, n=n),
        name="down_out",
        grid=(width // tile,),
        in_specs=in_specs,
        out_specs=out_specs,
        out_shape=out_shape,
        scratch_shapes=scratch,
        compiler_params=pltpu.CompilerParams(vmem_limit_bytes=VMEM_LIMIT, **params),
        cost_estimate=pl.CostEstimate(flops=2 * rows * depth * width, bytes_accessed=2 * depth * width + 2 * rows * depth + 4 * rows * width, transcendentals=0),
    )(*operands)


def gather_kernel(*refs, pieces, n, base):
    own, out_ref = refs[:pieces], refs[pieces]
    send_sem, recv_sem, own_sem = refs[pieces + 1:]
    me, meet, hop = ring_hops(own, out_ref, send_sem, recv_sem, n, base)
    meet()
    for i in range(pieces):
        for way in range(2):
            hop(0, i, way).start()
    for i in range(pieces):
        pltpu.make_async_copy(own[i], out_ref.at[me, base + i], own_sem.at[i]).start()
    for h in range(1, n):
        for i in range(pieces):
            for way in range(2):
                hop(h - 1, i, way).wait_recv()
                if h < n - 1:
                    hop(h, i, way).start()
    for h in range(n - 1):
        for i in range(pieces):
            for way in range(2):
                hop(h, i, way).wait_send()
    for i in range(pieces):
        pltpu.make_async_copy(own[i], out_ref.at[me, base + i], own_sem.at[i]).wait()


def gather_call(own, n, slots, base, collective_id):
    rows, width = own[0].shape
    pieces = len(own)
    moved = 2 * (n - 1) * pieces * rows * width
    return pl.pallas_call(
        functools.partial(gather_kernel, pieces=pieces, n=n, base=base),
        name="gather_tp",
        in_specs=[pl.BlockSpec(memory_space=pltpu.VMEM)] * pieces,
        out_specs=pl.BlockSpec(memory_space=pl.ANY),
        out_shape=jax.ShapeDtypeStruct((n, slots, rows, width), jnp.bfloat16),
        scratch_shapes=[
            pltpu.SemaphoreType.DMA((2, n - 1, pieces)),
            pltpu.SemaphoreType.DMA((2, n - 1, pieces)),
            pltpu.SemaphoreType.DMA((pieces,)),
        ],
        compiler_params=pltpu.CompilerParams(vmem_limit_bytes=VMEM_LIMIT, collective_id=collective_id, has_side_effects=True),
        cost_estimate=pl.CostEstimate(flops=moved * 1000, bytes_accessed=moved, transcendentals=0),
    )(*own)


def solution(mesh):
    sp_size = mesh.shape["sp"]
    tp_size = mesh.shape["tp"]
    row_spec = P(("rep", "sp"), None)
    cache_spec = P("rep", ("tp", "sp"), None)

    def layer_block(x_in, positions, norm_gain, w_q, w_k, w_v, w_o, w_gate, w_up, w_down):
        tok_local, width = x_in.shape
        cos, sin = rope_tables(positions)
        u, send = qkv_call(x_in, norm_gain[None, :], w_q, w_k, w_v, cos, sin, sp_size)
        recv = lax.all_to_all(send, "sp", 0, 0, tiled=True)
        hidden = gate_up_call(u, w_gate, w_up)
        recv, hidden = lax.optimization_barrier((recv, hidden))
        strip_rows = tok_local // (CHUNKS * tp_size)
        shard = tok_local // tp_size
        x_mine = lax.dynamic_slice_in_dim(x_in, lax.axis_index("tp") * shard, shard, axis=0)

        def finish(c, x_rows, total):
            return (x_rows[c * strip_rows:(c + 1) * strip_rows].astype(jnp.float32) + total).astype(jnp.bfloat16)

        sums, gathered, ids = [], [], iter(range(CHUNKS, 3 * CHUNKS))
        for c in range(CHUNKS):
            if c:
                recv, _ = lax.optimization_barrier((recv, partial))
            a_heads = flash_call(recv, c, tp_size, strip_rows)
            if c < LAG:
                partial, = down_out_call(hidden, a_heads, w_down, w_o, c, tp_size)
            else:
                total, a_heads = lax.optimization_barrier((sums[c - LAG], a_heads))
                own = finish(c - LAG, x_mine, total)
                partial, moved = down_out_call(hidden, a_heads, w_down, w_o, c, tp_size, own, next(ids))
                gathered.append(moved)
            sums.append(lax.psum_scatter(partial, "tp", scatter_dimension=0, tiled=True))
        waiting = range(CHUNKS - LAG, CHUNKS - 1)
        x_rest, _ = lax.optimization_barrier((x_mine, partial))
        early = gather_call([finish(c, x_rest, sums[c]) for c in waiting], tp_size, len(waiting), 0, next(ids))
        x_late, early = lax.optimization_barrier((x_rest, early))
        last = gather_call([finish(CHUNKS - 1, x_late, sums[-1])], tp_size, 1, 0, next(ids))
        y_out = jnp.concatenate([*gathered, early, last], axis=1).reshape(tok_local, width)
        k_all = recv[:, 1].reshape(sp_size * tok_local, 1, HEAD_DIM)
        v_all = recv[:, 2].reshape(sp_size * tok_local, 1, HEAD_DIM)
        return y_out, k_all, v_all

    return jax.shard_map(
        layer_block,
        mesh=mesh,
        in_specs=(row_spec, P(("rep", "sp")), P(None), P(None, "tp"), P(None, "tp"), P(None, "tp"), P("tp", None), P(None, "tp"), P(None, "tp"), P("tp", None)),
        out_specs=(row_spec, cache_spec, cache_spec),
        check_vma=False,
    )
```

```python
import functools
import math

import jax
import jax.numpy as jnp
from jax import lax
from jax.experimental import pallas as pl
from jax.experimental.pallas import tpu as pltpu
from jax.sharding import PartitionSpec as P

HEAD_DIM = 128
EPS = 1e-6
ROPE_BASE = 500000.0
SCORE_SCALE = HEAD_DIM ** -0.5
EXP2_SCALE = SCORE_SCALE * math.log2(math.e)
VMEM_LIMIT = 60 * 1024 * 1024
CHUNKS = 4
LAG = 2
MESH = pl.DeviceIdType.MESH
ROW_GROUP = 32


def rope_tables(positions):
    inv_freq = ROPE_BASE ** (-(jnp.arange(HEAD_DIM // 2, dtype=jnp.float32) * (2.0 / HEAD_DIM)))
    angles = positions.astype(jnp.float32)[:, None] * inv_freq[None, :]
    cos_tab, sin_tab = jnp.cos(angles), jnp.sin(angles)
    return jnp.concatenate([cos_tab, cos_tab], axis=-1), jnp.concatenate([-sin_tab, sin_tab], axis=-1)


def qkv_kernel(x_ref, g_ref, wq_ref, wk_ref, wv_ref, cos_ref, sin_ref, u_ref, send_ref):
    dests = send_ref.shape[0]
    kv_heads = wk_ref.shape[1] // HEAD_DIM
    repeat = dests // kv_heads
    x = x_ref[...].astype(jnp.float32)
    inv_rms = lax.rsqrt(jnp.mean(x * x, axis=-1, keepdims=True) + EPS)
    u_ref[...] = (x * inv_rms * g_ref[...]).astype(jnp.bfloat16)
    u = u_ref[...]
    cos, sin = cos_ref[...], sin_ref[...]

    def rotate(c):
        return (c * cos + pltpu.roll(c, HEAD_DIM // 2, 1) * sin).astype(jnp.bfloat16)

    q = jnp.dot(u, wq_ref[...], preferred_element_type=jnp.float32)
    for h in range(dests):
        send_ref[h, 0] = rotate(q[:, h * HEAD_DIM:(h + 1) * HEAD_DIM])
    k = jnp.dot(u, wk_ref[...], preferred_element_type=jnp.float32)
    v = jnp.dot(u, wv_ref[...], preferred_element_type=jnp.float32)
    for h in range(kv_heads):
        k_rot = rotate(k[:, h * HEAD_DIM:(h + 1) * HEAD_DIM])
        v_val = v[:, h * HEAD_DIM:(h + 1) * HEAD_DIM].astype(jnp.bfloat16)
        for r in range(repeat):
            send_ref[h * repeat + r, 1] = k_rot
            send_ref[h * repeat + r, 2] = v_val


def qkv_call(x_in, gain, w_q, w_k, w_v, cos, sin, dests):
    rows, width = x_in.shape
    tile = 256
    fixed = functools.partial(pl.BlockSpec, pipeline_mode=pl.Buffered(1))
    cols = w_q.shape[1] + w_k.shape[1] + w_v.shape[1]
    return pl.pallas_call(
        qkv_kernel,
        name="qkv_rope",
        grid=(rows // tile,),
        in_specs=[
            pl.BlockSpec((tile, width), lambda i: (i, 0)),
            fixed((1, width), lambda i: (0, 0)),
            fixed(w_q.shape, lambda i: (0, 0)),
            fixed(w_k.shape, lambda i: (0, 0)),
            fixed(w_v.shape, lambda i: (0, 0)),
            pl.BlockSpec((tile, HEAD_DIM), lambda i: (i, 0)),
            pl.BlockSpec((tile, HEAD_DIM), lambda i: (i, 0)),
        ],
        out_specs=[
            pl.BlockSpec((tile, width), lambda i: (i, 0)),
            pl.BlockSpec((dests, 3, tile, HEAD_DIM), lambda i: (0, 0, i, 0)),
        ],
        out_shape=[
            jax.ShapeDtypeStruct((rows, width), jnp.bfloat16),
            jax.ShapeDtypeStruct((dests, 3, rows, HEAD_DIM), jnp.bfloat16),
        ],
        compiler_params=pltpu.CompilerParams(vmem_limit_bytes=VMEM_LIMIT),
        cost_estimate=pl.CostEstimate(flops=2 * rows * width * cols, bytes_accessed=2 * (2 * rows * width + width * cols), transcendentals=0),
    )(x_in, gain, w_q, w_k, w_v, cos, sin)


def gate_up_kernel(u_ref, w1_ref, w3_ref, h_ref):
    u = u_ref[...]
    gate = jnp.dot(u, w1_ref[...], preferred_element_type=jnp.float32)
    up = jnp.dot(u, w3_ref[...], preferred_element_type=jnp.float32)
    h_ref[...] = (jax.nn.silu(gate) * up).astype(jnp.bfloat16)


def gate_up_call(u, w_gate, w_up):
    rows, width = u.shape
    cols = w_gate.shape[1]
    tile = 256
    return pl.pallas_call(
        gate_up_kernel,
        name="gate_up",
        grid=(cols // tile,),
        in_specs=[
            pl.BlockSpec((rows, width), lambda i: (0, 0), pipeline_mode=pl.Buffered(1)),
            pl.BlockSpec((width, tile), lambda i: (0, i)),
            pl.BlockSpec((width, tile), lambda i: (0, i)),
        ],
        out_specs=pl.BlockSpec((rows, tile), lambda i: (0, i)),
        out_shape=jax.ShapeDtypeStruct((rows, cols), jnp.bfloat16),
        compiler_params=pltpu.CompilerParams(vmem_limit_bytes=VMEM_LIMIT),
        cost_estimate=pl.CostEstimate(flops=4 * rows * width * cols, bytes_accessed=4 * width * cols + 2 * rows * (width + cols), transcendentals=rows * cols),
    )(u, w_gate, w_up)


def flash_kernel(q_ref, k_ref, v_ref, out_ref, tiles, s_buf, p_buf, alpha_buf, m_ref, l_ref, acc_ref, send_sem, recv_sem, own_sem, *, chunk, stride):
    srcs = k_ref.shape[0]
    here = pl.program_id(0)
    me = lax.axis_index("sp")
    src = lax.rem(me + 1 + here, srcs)

    def to_peer(dest):
        return pltpu.make_async_remote_copy(
            src_ref=tiles.at[dest], dst_ref=out_ref.at[me], send_sem=send_sem.at[dest], recv_sem=recv_sem.at[me],
            device_id={"sp": dest}, device_id_type=MESH)

    def to_self():
        return pltpu.make_async_copy(tiles.at[me], out_ref.at[me], own_sem)

    @pl.when(here == 0)
    def _():
        barrier = pltpu.get_barrier_semaphore()
        for j in range(1, srcs):
            pl.semaphore_signal(barrier, inc=1, device_id={"sp": lax.rem(me + j, srcs)}, device_id_type=MESH)
        pl.semaphore_wait(barrier, srcs - 1)

    @pl.when(here > 0)
    def _():
        to_peer(lax.rem(me + here, srcs)).start()

    strips, strip_rows = q_ref.shape[2], q_ref.shape[3]
    rows = strips * strip_rows
    cols = k_ref.shape[2]
    q = q_ref[src, 0].reshape(rows, HEAD_DIM)

    def source_of(t):
        return jnp.where(t == 0, src, t - 1)

    def scores(t, slot):
        s_buf[slot] = lax.dot_general(q, k_ref[source_of(t), 0], (((1,), (1,)), ((), ())), preferred_element_type=jnp.float32)

    def soften(slot, masked):
        for r in range(0, rows, ROW_GROUP):
            group = pl.ds(r, ROW_GROUP)
            s = [s_buf[slot, group, pl.ds(g, HEAD_DIM)] for g in range(0, cols, HEAD_DIM)]
            if masked:
                row_id = lax.broadcasted_iota(jnp.int32, (ROW_GROUP, HEAD_DIM), 0) + (r // strip_rows * stride + chunk * strip_rows + r % strip_rows)
                col_id = lax.broadcasted_iota(jnp.int32, (ROW_GROUP, HEAD_DIM), 1)
                s = [jnp.where(col_id + g * HEAD_DIM <= row_id, s_g, -jnp.inf) for g, s_g in enumerate(s)]
            top = s[0]
            for s_g in s[1:]:
                top = jnp.maximum(top, s_g)
            top = jnp.broadcast_to(jnp.max(top, axis=1, keepdims=True), (ROW_GROUP, HEAD_DIM))
            if masked:
                alpha_buf[slot, group] = jnp.ones_like(top)
                total = jnp.zeros_like(top)
            else:
                m_old = m_ref[group]
                top = jnp.maximum(m_old, top)
                alpha = jnp.exp2((m_old - top) * EXP2_SCALE)
                alpha_buf[slot, group] = alpha
                total = l_ref[group] * alpha
            m_ref[group] = top
            for g, s_g in enumerate(s):
                p = jnp.exp2((s_g - top) * EXP2_SCALE)
                total = total + p
                p_buf[slot, group, pl.ds(g * HEAD_DIM, HEAD_DIM)] = p.astype(jnp.bfloat16)
            l_ref[group] = total

    def values(t, slot):
        acc_ref[...] = acc_ref[...] * alpha_buf[slot] + jnp.dot(p_buf[slot], v_ref[source_of(t), 0], preferred_element_type=jnp.float32)

    acc_ref[...] = jnp.zeros_like(acc_ref)
    scores(0, 0)
    scores(jnp.minimum(src, 1), 1)
    soften(0, True)

    def step(t, carry):
        for now in range(2):
            @pl.when(t % 2 == now)
            def _():
                scores(jnp.minimum(t + 1, src), 1 - now)
                soften(now, False)
                values(t - 1, 1 - now)
        return carry

    lax.fori_loop(1, src + 1, step, 0)
    for now in range(2):
        @pl.when(src % 2 == now)
        def _():
            values(src, now)
    tiles[src] = (acc_ref[...] / jnp.sum(l_ref[...], axis=1, keepdims=True)).astype(jnp.bfloat16)

    @pl.when(here == srcs - 1)
    def _():
        to_self().start()
        for j in range(1, srcs):
            to_peer(lax.rem(me + j, srcs)).wait_send()
        to_self().wait()
        for j in range(1, srcs):
            peer = lax.rem(me + j, srcs)
            pltpu.make_async_remote_copy(
                src_ref=tiles.at[0], dst_ref=out_ref.at[peer], send_sem=send_sem.at[0], recv_sem=recv_sem.at[peer],
                device_id={"sp": peer}, device_id_type=MESH).wait_recv()


def flash_call(recv, chunk, strips, strip_rows):
    srcs, _, per_src, _ = recv.shape
    rows = strips * strip_rows
    work = srcs * rows * (srcs * per_src // 2)
    by_strip = recv.reshape(srcs, 3, strips, per_src // strips, HEAD_DIM)
    return pl.pallas_call(
        functools.partial(flash_kernel, chunk=chunk, stride=per_src // strips),
        name="flash",
        grid=(srcs,),
        in_specs=[
            pl.BlockSpec((srcs, 1, strips, strip_rows, HEAD_DIM), lambda s: (0, 0, 0, chunk, 0), pipeline_mode=pl.Buffered(1)),
            pl.BlockSpec((srcs, 1, per_src, HEAD_DIM), lambda s: (0, 1, 0, 0), pipeline_mode=pl.Buffered(1)),
            pl.BlockSpec((srcs, 1, per_src, HEAD_DIM), lambda s: (0, 2, 0, 0), pipeline_mode=pl.Buffered(1)),
        ],
        out_specs=pl.BlockSpec(memory_space=pl.ANY),
        out_shape=jax.ShapeDtypeStruct((srcs, rows, HEAD_DIM), jnp.bfloat16),
        scratch_shapes=[
            pltpu.VMEM((srcs, rows, HEAD_DIM), jnp.bfloat16),
            pltpu.VMEM((2, rows, per_src), jnp.float32),
            pltpu.VMEM((2, rows, per_src), jnp.bfloat16),
            pltpu.VMEM((2, rows, HEAD_DIM), jnp.float32),
            pltpu.VMEM((rows, HEAD_DIM), jnp.float32),
            pltpu.VMEM((rows, HEAD_DIM), jnp.float32),
            pltpu.VMEM((rows, HEAD_DIM), jnp.float32),
            pltpu.SemaphoreType.DMA((srcs,)),
            pltpu.SemaphoreType.DMA((srcs,)),
            pltpu.SemaphoreType.DMA,
        ],
        compiler_params=pltpu.CompilerParams(vmem_limit_bytes=VMEM_LIMIT, collective_id=chunk, has_side_effects=True),
        cost_estimate=pl.CostEstimate(flops=8 * work * HEAD_DIM, bytes_accessed=6 * srcs * per_src * HEAD_DIM, transcendentals=work),
    )(by_strip, recv, recv)


def ring_hops(own, out_ref, send_sem, recv_sem, n, base):
    me = lax.axis_index("tp")
    right, left = lax.rem(me + 1, n), lax.rem(me + n - 1, n)
    half = own[0].shape[0] // 2

    def meet():
        barrier = pltpu.get_barrier_semaphore()
        for peer in (left, right):
            pl.semaphore_signal(barrier, inc=1, device_id={"tp": peer}, device_id_type=MESH)
        pl.semaphore_wait(barrier, 2)

    def hop(h, i, way):
        owner = lax.rem(me + (n - h if way == 0 else h), n)
        rows = pl.ds(way * half, half)
        place = out_ref.at[owner, base + i, rows]
        return pltpu.make_async_remote_copy(
            src_ref=own[i].at[rows] if h == 0 else place, dst_ref=place,
            send_sem=send_sem.at[way, h, i], recv_sem=recv_sem.at[way, h, i],
            device_id={"tp": right if way == 0 else left}, device_id_type=MESH)

    return me, meet, hop


def down_out_kernel(*refs, n):
    h_ref, a_ref, wd_ref, wo_ref = refs[:4]
    step, last = pl.program_id(0), pl.num_programs(0) - 1
    if n:
        own, o_ref, gathered, send_sem, recv_sem, own_sem = refs[4:]
        me, meet, hop = ring_hops([own], gathered, send_sem, recv_sem, n, 0)

        def keep():
            return pltpu.make_async_copy(own, gathered.at[me, 0], own_sem)

        @pl.when(step == 0)
        def _():
            meet()
            for way in range(2):
                hop(0, 0, way).start()
            keep().start()

        for h in range(1, n - 1):
            @pl.when(step == jnp.minimum(1 + 2 * h, last))
            def _():
                for way in range(2):
                    hop(h - 1, 0, way).wait_recv()
                    hop(h, 0, way).start()
    else:
        o_ref, = refs[4:]
    a = jnp.concatenate([a_ref[i] for i in range(a_ref.shape[0])], axis=1)
    attn = jnp.dot(a, wo_ref[...], preferred_element_type=jnp.float32)
    hidden = h_ref[...].reshape(a.shape[0], h_ref.shape[2])
    o_ref[...] = attn + jnp.dot(hidden, wd_ref[...], preferred_element_type=jnp.float32)
    if n:
        @pl.when(step == last)
        def _():
            for way in range(2):
                hop(n - 2, 0, way).wait_recv()
                for h in range(n - 1):
                    hop(h, 0, way).wait_send()
            keep().wait()


def down_out_call(hidden, a_heads, w_down, w_o, chunk, strips, own=None, collective_id=None):
    heads, rows, _ = a_heads.shape
    ff, width = w_down.shape
    tile = 512
    depth = ff + w_o.shape[0]
    in_specs = [
        pl.BlockSpec((strips, rows // strips, ff), lambda i: (0, chunk, 0), pipeline_mode=pl.Buffered(1)),
        pl.BlockSpec((heads, rows, HEAD_DIM), lambda i: (0, 0, 0), pipeline_mode=pl.Buffered(1)),
        pl.BlockSpec((ff, tile), lambda i: (0, i)),
        pl.BlockSpec((w_o.shape[0], tile), lambda i: (0, i)),
    ]
    out_specs = [pl.BlockSpec((rows, tile), lambda i: (0, i))]
    out_shape = [jax.ShapeDtypeStruct((rows, width), jnp.float32)]
    operands = [hidden.reshape(strips, hidden.shape[0] // strips, ff), a_heads, w_down, w_o]
    scratch, n, params = [], 0, {}
    if own is not None:
        n = strips
        in_specs.append(pl.BlockSpec(own.shape, lambda i: (0, 0), pipeline_mode=pl.Buffered(1)))
        out_specs.append(pl.BlockSpec(memory_space=pl.ANY))
        out_shape.append(jax.ShapeDtypeStruct((n, 1, *own.shape), own.dtype))
        operands.append(own)
        scratch = [pltpu.SemaphoreType.DMA((2, n - 1, 1)), pltpu.SemaphoreType.DMA((2, n - 1, 1)), pltpu.SemaphoreType.DMA]
        params = {"collective_id": collective_id, "has_side_effects": True}
    return pl.pallas_call(
        functools.partial(down_out_kernel, n=n),
        name="down_out",
        grid=(width // tile,),
        in_specs=in_specs,
        out_specs=out_specs,
        out_shape=out_shape,
        scratch_shapes=scratch,
        compiler_params=pltpu.CompilerParams(vmem_limit_bytes=VMEM_LIMIT, **params),
        cost_estimate=pl.CostEstimate(flops=2 * rows * depth * width, bytes_accessed=2 * depth * width + 2 * rows * depth + 4 * rows * width, transcendentals=0),
    )(*operands)


def gather_kernel(*refs, pieces, n, base):
    own, out_ref = refs[:pieces], refs[pieces]
    send_sem, recv_sem, own_sem = refs[pieces + 1:]
    me, meet, hop = ring_hops(own, out_ref, send_sem, recv_sem, n, base)
    meet()
    for i in range(pieces):
        for way in range(2):
            hop(0, i, way).start()
    for i in range(pieces):
        pltpu.make_async_copy(own[i], out_ref.at[me, base + i], own_sem.at[i]).start()
    for h in range(1, n):
        for i in range(pieces):
            for way in range(2):
                hop(h - 1, i, way).wait_recv()
                if h < n - 1:
                    hop(h, i, way).start()
    for h in range(n - 1):
        for i in range(pieces):
            for way in range(2):
                hop(h, i, way).wait_send()
    for i in range(pieces):
        pltpu.make_async_copy(own[i], out_ref.at[me, base + i], own_sem.at[i]).wait()


def gather_call(own, n, slots, base, collective_id):
    rows, width = own[0].shape
    pieces = len(own)
    moved = 2 * (n - 1) * pieces * rows * width
    return pl.pallas_call(
        functools.partial(gather_kernel, pieces=pieces, n=n, base=base),
        name="gather_tp",
        in_specs=[pl.BlockSpec(memory_space=pltpu.VMEM)] * pieces,
        out_specs=pl.BlockSpec(memory_space=pl.ANY),
        out_shape=jax.ShapeDtypeStruct((n, slots, rows, width), jnp.bfloat16),
        scratch_shapes=[
            pltpu.SemaphoreType.DMA((2, n - 1, pieces)),
            pltpu.SemaphoreType.DMA((2, n - 1, pieces)),
            pltpu.SemaphoreType.DMA((pieces,)),
        ],
        compiler_params=pltpu.CompilerParams(vmem_limit_bytes=VMEM_LIMIT, collective_id=collective_id, has_side_effects=True),
        cost_estimate=pl.CostEstimate(flops=moved * 1000, bytes_accessed=moved, transcendentals=0),
    )(*own)


def solution(mesh):
    sp_size = mesh.shape["sp"]
    tp_size = mesh.shape["tp"]
    row_spec = P(("rep", "sp"), None)
    cache_spec = P("rep", ("tp", "sp"), None)

    def layer_block(x_in, positions, norm_gain, w_q, w_k, w_v, w_o, w_gate, w_up, w_down):
        tok_local, width = x_in.shape
        cos, sin = rope_tables(positions)
        u, send = qkv_call(x_in, norm_gain[None, :], w_q, w_k, w_v, cos, sin, sp_size)
        recv = lax.all_to_all(send, "sp", 0, 0, tiled=True)
        hidden = gate_up_call(u, w_gate, w_up)
        recv, hidden = lax.optimization_barrier((recv, hidden))
        strip_rows = tok_local // (CHUNKS * tp_size)
        shard = tok_local // tp_size
        x_mine = lax.dynamic_slice_in_dim(x_in, lax.axis_index("tp") * shard, shard, axis=0)

        def finish(c, x_rows, total):
            return (x_rows[c * strip_rows:(c + 1) * strip_rows].astype(jnp.float32) + total).astype(jnp.bfloat16)

        sums, gathered, ids = [], [], iter(range(CHUNKS, 3 * CHUNKS))
        for c in range(CHUNKS):
            if c:
                recv, _ = lax.optimization_barrier((recv, partial))
            a_heads = flash_call(recv, c, tp_size, strip_rows)
            if c < LAG:
                partial, = down_out_call(hidden, a_heads, w_down, w_o, c, tp_size)
            else:
                total, a_heads = lax.optimization_barrier((sums[c - LAG], a_heads))
                own = finish(c - LAG, x_mine, total)
                partial, moved = down_out_call(hidden, a_heads, w_down, w_o, c, tp_size, own, next(ids))
                gathered.append(moved)
            sums.append(lax.psum_scatter(partial, "tp", scatter_dimension=0, tiled=True))
        waiting = range(CHUNKS - LAG, CHUNKS - 1)
        x_rest, _ = lax.optimization_barrier((x_mine, partial))
        early = gather_call([finish(c, x_rest, sums[c]) for c in waiting], tp_size, len(waiting), 0, next(ids))
        x_rest, early, recv = lax.optimization_barrier((x_rest, early, recv))
        k_all = recv[:, 1].reshape(sp_size * tok_local, 1, HEAD_DIM)
        v_all = recv[:, 2].reshape(sp_size * tok_local, 1, HEAD_DIM)
        x_late, k_all, v_all = lax.optimization_barrier((x_rest, k_all, v_all))
        last = gather_call([finish(CHUNKS - 1, x_late, sums[-1])], tp_size, 1, 0, next(ids))
        y_out = jnp.concatenate([*gathered, early, last], axis=1).reshape(tok_local, width)
        return y_out, k_all, v_all

    return jax.shard_map(
        layer_block,
        mesh=mesh,
        in_specs=(row_spec, P(("rep", "sp")), P(None), P(None, "tp"), P(None, "tp"), P(None, "tp"), P("tp", None), P(None, "tp"), P(None, "tp"), P("tp", None)),
        out_specs=(row_spec, cache_spec, cache_spec),
        check_vma=False,
    )
```
